32 devices in a mesh: blk: 16 (over z, y, core), rows: 2 (over x).
Axes of the slice: x: 2, y: 2, z: 4, core: 2. Of those that a mesh axis runs over, the one named last changes fastest.
Arguments:
- columns: float32 [2048, 1280], P('blk', 'rows'), may hold values from -9 to 9
- right_factor: float32 [2048, 512], P('blk', 'rows'), may hold values from -6 to 6
Outputs:
- new_columns: float32 [2048, 1280], P('blk', 'rows')
- new_factor: float32 [2048, 512], P('blk', 'rows')
The draws below stay inside these ranges and needn't reach their ends.
All inputs are finite; a program needn't handle non-finite values.
Results may differ from the reference program's by a relative error of at most 0.0003.
Values sent between devices are 32-bit elements; how exact they have to be, the bound alone decides.
A program may use at most 64 MiB of HBM per device.

```python
import jax
import jax.numpy as jnp
from jax import lax

BLOCK = 64
STEPS = 6
ORDER = 2048
ROWS = 1280
FACTOR_ROWS = 512
N_BLK = 16


def draw_columns(key, part):
    noise_key, left_key, right_key = jax.random.split(jax.random.fold_in(key, 17), 3)
    noise_part = jax.random.truncated_normal(noise_key, -4.0, 4.0, (ORDER, ROWS), jnp.float32)
    weights = jnp.array([0.2, 0.15, 0.1, 0.07], jnp.float32)
    left_part = jax.random.truncated_normal(left_key, -3.0, 3.0, (ORDER, 4), jnp.float32) * weights
    right_part = jax.random.truncated_normal(right_key, -3.0, 3.0, (4, ROWS), jnp.float32)
    return noise_part + jnp.dot(left_part, right_part, precision=lax.Precision.HIGHEST)


def level_of(key, extent, shards, low, top_value):
    level = 1.0
    for position, shards_of in shards:
        draws = jax.random.uniform(jax.random.fold_in(jax.random.fold_in(key, 6), position), (shards_of,), jnp.float32, low / len(shards), top_value / len(shards))
        level = level * jnp.repeat(jnp.exp(draws), extent[position] // shards_of).reshape((-1,) + (1,) * (len(extent) - 1 - position))
    return level


def normal_values(rng, shape, spread, limit, cuts=(), kind=jnp.bfloat16):
    drawn = spread * jax.random.normal(rng, shape, jnp.float32)
    if cuts:
        drawn = drawn * level_of(rng, shape, cuts, -0.22, 0.18)
    return jnp.clip(drawn, -limit, limit).astype(kind)


def setup_inputs(seed: int = 0) -> dict:
    seeds = jax.random.split(jax.random.key(seed), 3)
    return {
        "columns": draw_columns(jax.random.fold_in(seeds[2], 71), 0),
        "right_factor": normal_values(seeds[1], (ORDER, FACTOR_ROWS), 1.0, 6.0, ((0, 16), (1, 2)), jnp.float32),
    }


HIGHEST_PREC = lax.Precision.HIGHEST

def orth_factor(square):
    lower_factor = jnp.linalg.cholesky(jnp.dot(square.T, square, precision=HIGHEST_PREC))
    return jax.scipy.linalg.solve_triangular(lower_factor, square.T, lower=True).T

def rotation(pair_gram):
    first_turn = orth_factor(pair_gram)
    return orth_factor(jnp.dot(pair_gram, first_turn, precision=HIGHEST_PREC))

def pass_moving(blocks):
    return jnp.concatenate([blocks[:, :BLOCK], jnp.roll(blocks[:, BLOCK:], 1, axis=0)], axis=1)

def reference(columns, right_factor):
    column_pairs = columns.reshape(N_BLK, 2 * BLOCK, ROWS)
    factor_pairs = right_factor.reshape(N_BLK, 2 * BLOCK, FACTOR_ROWS)

    def advance(current, unused):
        column_pairs, factor_pairs = current
        pair_grams = jnp.einsum('pim,pjm->pij', column_pairs, column_pairs, precision=HIGHEST_PREC)
        rotations = jax.vmap(rotation)(pair_grams)
        column_pairs = jnp.einsum('pij,pim->pjm', rotations, column_pairs, precision=HIGHEST_PREC)
        factor_pairs = jnp.einsum('pij,pim->pjm', rotations, factor_pairs, precision=HIGHEST_PREC)
        return ((pass_moving(column_pairs), pass_moving(factor_pairs)), None)
    final_state, unused = lax.scan(advance, (column_pairs, factor_pairs), None, length=STEPS)
    return (final_state[0].reshape(ORDER, ROWS), final_state[1].reshape(ORDER, FACTOR_ROWS))
```

```python
import jax
import jax.numpy as jnp
from jax import lax
from jax.sharding import PartitionSpec as P

STEPS = 6


HIGHEST_PREC = lax.Precision.HIGHEST


def shifted(block, axis, distance):
    devices = range(lax.axis_size(axis))
    route = [((i - distance) % len(devices), i) for i in devices]
    return lax.ppermute(block, axis, route)


def rotation(pair_gram):
    first = jnp.linalg.cholesky(jnp.dot(pair_gram, pair_gram, precision=HIGHEST_PREC))
    second = jnp.linalg.cholesky(jnp.dot(first.T, first, precision=HIGHEST_PREC))
    return jax.scipy.linalg.solve_triangular(second, first.T, lower=True).T


def gram_of(upper_rows, lower_rows):
    return lax.dot_general(upper_rows, lower_rows, (((1,), (1,)), ((), ())), precision=HIGHEST_PREC)


def rotate(rotation_matrix, blocks):
    return lax.dot_general(
        rotation_matrix, blocks, (((0,), (0,)), ((), ())), precision=HIGHEST_PREC
    )


def body(columns, right_factor):
    block_width = columns.shape[0] // 2
    stay_gram, moving_gram = lax.psum(
        (
            gram_of(columns[:block_width], columns[:block_width]),
            gram_of(columns[block_width:], columns[block_width:]),
        ),
        "rows",
    )

    def advance_cross(step_index, loop_state):
        column_pair, factor_pair, stay_gram, moving_gram = loop_state
        cross_term = lax.psum(gram_of(column_pair[:block_width], column_pair[block_width:]), "rows")
        upper_half = jnp.concatenate([stay_gram, cross_term], 1)
        lower_half = jnp.concatenate([cross_term.T, moving_gram], 1)
        pair_gram = jnp.concatenate([upper_half, lower_half], 0)
        rotation_matrix = rotation(pair_gram)
        column_pair = rotate(rotation_matrix, column_pair)
        factor_pair = rotate(rotation_matrix, factor_pair)
        rotated_gram = rotate(
            rotation_matrix, jnp.dot(pair_gram, rotation_matrix, precision=HIGHEST_PREC)
        )
        arrived = shifted(
            (
                column_pair[block_width:],
                factor_pair[block_width:],
                rotated_gram[block_width:, block_width:],
            ),
            "blk",
            1,
        )
        return (
            jnp.concatenate([column_pair[:block_width], arrived[0]], 0),
            jnp.concatenate([factor_pair[:block_width], arrived[1]], 0),
            rotated_gram[:block_width, :block_width],
            arrived[2],
        )

    result = lax.fori_loop(0, STEPS, advance_cross, (columns, right_factor, stay_gram, moving_gram))
    return (result[0], result[1])


def solution(mesh):
    return jax.shard_map(
        body,
        mesh=mesh,
        in_specs=(P("blk", "rows"), P("blk", "rows")),
        out_specs=(P("blk", "rows"), P("blk", "rows")),
        check_vma=False,
    )
```

```python
import functools

import jax
import jax.numpy as jnp
from jax import lax
from jax.experimental import pallas as pl
from jax.experimental.pallas import tpu as pltpu
from jax.sharding import PartitionSpec as P

STEPS = 6
PANEL = 16

HIGHEST_PREC = lax.Precision.HIGHEST


def dot_nn(a, b):
    return lax.dot_general(
        a, b, (((1,), (0,)), ((), ())), precision=HIGHEST_PREC, preferred_element_type=jnp.float32
    )


def dot_nt(a, b):
    return lax.dot_general(
        a, b, (((1,), (1,)), ((), ())), precision=HIGHEST_PREC, preferred_element_type=jnp.float32
    )


def dot_tn(a, b):
    return lax.dot_general(
        a, b, (((0,), (0,)), ((), ())), precision=HIGHEST_PREC, preferred_element_type=jnp.float32
    )


def eliminate(work):
    order, width = work.shape
    panels = order // PANEL
    for panel in range(panels):
        low = panel * PANEL
        high = low + PANEL
        end = min(high + PANEL, order)
        rows = work[low:high, :]
        below = work[high:end, :] if end > high else None
        spread = [
            jnp.broadcast_to(rows[:, low + k : low + k + 1], (PANEL, 128)) for k in range(PANEL)
        ]
        spread_below = None
        if below is not None:
            spread_below = [
                jnp.broadcast_to(below[:, low + k : low + k + 1], (end - high, 128))
                for k in range(PANEL)
            ]
        done = []
        for j in range(PANEL):
            scale = lax.rsqrt(spread[j][j : j + 1, :])
            column = spread[j] * scale
            wide = jnp.concatenate([scale] * (width // 128), axis=1)
            pivot_row = rows[j : j + 1, :] * wide
            done.append(pivot_row)
            wide_column = jnp.concatenate([column] * (width // 128), axis=1)
            if j + 1 < PANEL:
                rows = rows - wide_column * pivot_row
            if below is not None:
                column_below = spread_below[j] * scale
                wide_below = jnp.concatenate([column_below] * (width // 128), axis=1)
                below = below - wide_below * pivot_row
            for k in range(j + 1, PANEL):
                head = spread[k][j : j + 1, :] * scale
                spread[k] = spread[k] - column * head
                if below is not None:
                    spread_below[k] = spread_below[k] - column_below * head
        finished = jnp.concatenate(done, axis=0)
        work[low:high, :] = finished
        if below is not None:
            work[high:end, :] = below
        if end < order:
            work[end:, :] = work[end:, :] - dot_tn(finished[:, end:order], finished)


def step_kernel(
    stay_cols, stay_fac, moving, stay_gram, cross, peer_cross, out_stay, out_fac, out_moving, out_gram,
    gram, work, solve,
):
    half, col_width = stay_cols.shape
    order = 2 * half
    fac_width = stay_fac.shape[1]
    gram_at = col_width + fac_width
    cross_term = cross[...] + peer_cross[...]
    gram[:half, :half] = stay_gram[...]
    gram[:half, half:] = cross_term
    gram[half:, :half] = cross_term.T
    gram[half:, half:] = moving[:, gram_at + half : gram_at + order]
    g = gram[...]
    work[...] = dot_nn(g, g)
    eliminate(work)
    upper = work[...]
    keep = lax.broadcasted_iota(jnp.int32, upper.shape, 0) <= lax.broadcasted_iota(
        jnp.int32, upper.shape, 1
    )
    upper = jnp.where(keep, upper, 0.0)
    solve[:, :order] = dot_nt(upper, upper)
    solve[:, order:] = upper
    eliminate(solve)
    turn = solve[:, order:]
    top, low = turn[:half], turn[half:]
    columns = jnp.concatenate([stay_cols[...], moving[:, :col_width]], axis=0)
    out_moving[:, :col_width] = dot_nn(low, columns)
    factors = jnp.concatenate([stay_fac[...], moving[:, col_width:gram_at]], axis=0)
    out_moving[:, col_width:gram_at] = dot_nn(low, factors)
    new_gram = dot_nt(dot_nn(turn, g), turn)
    out_moving[:, gram_at:] = new_gram[half:]
    out_gram[...] = new_gram[:half, :half]
    out_stay[...] = dot_nn(top, columns)
    out_fac[...] = dot_nn(top, factors)


def one_step(*operands):
    stay_cols, stay_fac, moving, stay_gram, cross, peer_cross = operands
    order = 2 * stay_cols.shape[0]
    shapes = [stay_cols, stay_fac, moving, stay_gram]
    return pl.pallas_call(
        step_kernel,
        out_shape=[jax.ShapeDtypeStruct(a.shape, a.dtype) for a in shapes],
        in_specs=[pl.BlockSpec(memory_space=pltpu.VMEM)] * 6,
        out_specs=[pl.BlockSpec(memory_space=pltpu.VMEM)] * 4,
        scratch_shapes=[
            pltpu.VMEM((order, order), jnp.float32),
            pltpu.VMEM((order, order), jnp.float32),
            pltpu.VMEM((order, 2 * order), jnp.float32),
        ],
        name="turn",
    )(*operands)


def summands(part):
    if lax.axis_size("rows") == 2:
        return part, lax.ppermute(part, "rows", [(0, 1), (1, 0)])
    return lax.psum(part, "rows"), jnp.zeros_like(part)


def gram_of(upper_rows, lower_rows):
    return dot_nt(upper_rows, lower_rows)


def body(columns, right_factor):
    half = columns.shape[0] // 2
    col_width = columns.shape[1]
    ring = lax.axis_size("blk")
    route = [((i - 1) % ring, i) for i in range(ring)]
    stay_gram, moving_gram = lax.psum(
        (gram_of(columns[:half], columns[:half]), gram_of(columns[half:], columns[half:])), "rows"
    )
    moving = jnp.concatenate(
        [columns[half:], right_factor[half:], moving_gram, moving_gram], axis=1
    )
    state = (columns[:half], right_factor[:half], moving, stay_gram)

    def advance(step_index, state):
        stay_cols, stay_fac, moving, stay_gram = state
        cross = gram_of(stay_cols, moving[:, :col_width])
        stay_cols, stay_fac, moving, stay_gram = one_step(
            stay_cols, stay_fac, moving, stay_gram, *summands(cross)
        )
        return stay_cols, stay_fac, lax.ppermute(moving, "blk", route), stay_gram

    stay_cols, stay_fac, moving, _ = lax.fori_loop(0, STEPS, advance, state)
    fac_end = col_width + right_factor.shape[1]
    return (
        jnp.concatenate([stay_cols, moving[:, :col_width]], axis=0),
        jnp.concatenate([stay_fac, moving[:, col_width:fac_end]], axis=0),
    )


def solution(mesh):
    return jax.shard_map(
        body,
        mesh=mesh,
        in_specs=(P("blk", "rows"), P("blk", "rows")),
        out_specs=(P("blk", "rows"), P("blk", "rows")),
        check_vma=False,
    )
```

```python
import jax
import jax.numpy as jnp
from jax import lax
from jax.experimental import pallas as pl
from jax.experimental.pallas import tpu as pltpu
from jax.sharding import PartitionSpec as P

STEPS = 6
PANEL = 16
LANES = 128
MESH = pl.DeviceIdType.MESH

HIGHEST_PREC = lax.Precision.HIGHEST


def dot_nn(a, b):
    return lax.dot_general(
        a, b, (((1,), (0,)), ((), ())), precision=HIGHEST_PREC, preferred_element_type=jnp.float32
    )


def dot_nt(a, b):
    return lax.dot_general(
        a, b, (((1,), (1,)), ((), ())), precision=HIGHEST_PREC, preferred_element_type=jnp.float32
    )


def dot_tn(a, b):
    return lax.dot_general(
        a, b, (((0,), (0,)), ((), ())), precision=HIGHEST_PREC, preferred_element_type=jnp.float32
    )


def eliminate(work):
    order, width = work.shape
    panels = order // PANEL
    for panel in range(panels):
        low = panel * PANEL
        high = low + PANEL
        end = min(high + PANEL, order)
        rows = work[low:high, :]
        below = work[high:end, :] if end > high else None
        spread = [
            jnp.broadcast_to(rows[:, low + k : low + k + 1], (PANEL, 128)) for k in range(PANEL)
        ]
        spread_below = None
        if below is not None:
            spread_below = [
                jnp.broadcast_to(below[:, low + k : low + k + 1], (end - high, 128))
                for k in range(PANEL)
            ]
        done = []
        for j in range(PANEL):
            scale = lax.rsqrt(spread[j][j : j + 1, :])
            column = spread[j] * scale
            wide = jnp.concatenate([scale] * (width // 128), axis=1)
            pivot_row = rows[j : j + 1, :] * wide
            done.append(pivot_row)
            wide_column = jnp.concatenate([column] * (width // 128), axis=1)
            if j + 1 < PANEL:
                rows = rows - wide_column * pivot_row
            if below is not None:
                column_below = spread_below[j] * scale
                wide_below = jnp.concatenate([column_below] * (width // 128), axis=1)
                below = below - wide_below * pivot_row
            for k in range(j + 1, PANEL):
                head = spread[k][j : j + 1, :] * scale
                spread[k] = spread[k] - column * head
                if below is not None:
                    spread_below[k] = spread_below[k] - column_below * head
        finished = jnp.concatenate(done, axis=0)
        work[low:high, :] = finished
        if below is not None:
            work[high:end, :] = below
        if end < order:
            work[end:, :] = work[end:, :] - dot_tn(finished[:, end:order], finished)


def lanes(chunk):
    return slice(chunk * LANES, (chunk + 1) * LANES)


def cycle_kernel(
    columns, right_factor, new_columns, new_factor, stay, sent, held, grams, stay_gram, gram, work,
    solve, sent_sem, held_sem, gram_sent_sem, gram_sem,
):
    half = columns.shape[0] // 2
    order = 2 * half
    col_chunks = columns.shape[1] // LANES
    chunks = col_chunks + right_factor.shape[1] // LANES
    ring, peers = lax.axis_size("blk"), lax.axis_size("rows")
    place, row_place = lax.axis_index("blk"), lax.axis_index("rows")
    right, left = lax.rem(place + 1, ring), lax.rem(place + ring - 1, ring)

    barrier = pltpu.get_barrier_semaphore()
    for neighbour in (left, right):
        pl.semaphore_signal(barrier, inc=1, device_id={"blk": neighbour}, device_id_type=MESH)
    for off in range(1, peers):
        peer = lax.rem(row_place + off, peers)
        pl.semaphore_signal(barrier, inc=1, device_id={"rows": peer}, device_id_type=MESH)

    def gram_copy(step, off, first):
        part = grams.at[step, row_place]
        if not first:
            part = part.at[pl.ds(half, half)]
        return pltpu.make_async_remote_copy(
            src_ref=part,
            dst_ref=part,
            send_sem=gram_sent_sem.at[step, off - 1],
            recv_sem=gram_sem.at[step, off - 1],
            device_id={"rows": lax.rem(row_place + off, peers)},
            device_id_type=MESH,
        )

    def ring_copy(step, chunk):
        return pltpu.make_async_remote_copy(
            src_ref=sent.at[step, chunk],
            dst_ref=held.at[step + 1, chunk],
            send_sem=sent_sem.at[step, chunk],
            recv_sem=held_sem.at[step, chunk],
            device_id={"blk": right},
            device_id_type=MESH,
        )

    total = jnp.zeros((order, order), jnp.float32)
    for chunk in range(chunks):
        source = columns if chunk < col_chunks else right_factor
        at = lanes(chunk if chunk < col_chunks else chunk - col_chunks)
        stay[chunk] = source[:half, at]
        held[0, chunk] = source[half:, at]
        if chunk < col_chunks:
            total = total + dot_nt(source[:, at], source[:, at])
    grams[0, row_place] = total
    pl.semaphore_wait(barrier, 2 + peers - 1)
    for off in range(1, peers):
        gram_copy(0, off, True).start()
    for off in range(1, peers):
        gram_copy(0, off, True).wait()
    first_gram = grams[0, 0, :half, :half]
    for peer in range(1, peers):
        first_gram = first_gram + grams[0, peer, :half, :half]
    stay_gram[...] = first_gram

    def advance(step, carry):
        @pl.when(step > 0)
        def _():
            for off in range(1, peers):
                gram_copy(step, off, False).wait()

        lower = grams[step, 0, half:, :]
        for peer in range(1, peers):
            lower = lower + grams[step, peer, half:, :]
        gram[:half, :half] = stay_gram[...]
        gram[:half, half:] = lower[:, :half].T
        gram[half:, :] = lower
        g = gram[...]
        work[...] = dot_nn(g, g)
        eliminate(work)
        upper = work[...]
        keep = lax.broadcasted_iota(jnp.int32, upper.shape, 0) <= lax.broadcasted_iota(
            jnp.int32, upper.shape, 1
        )
        upper = jnp.where(keep, upper, 0.0)
        solve[:, :order] = dot_nt(upper, upper)
        solve[:, order:] = upper
        eliminate(solve)
        turn = solve[:, order:]
        top, low = turn[:half], turn[half:]

        def pair(chunk):
            return jnp.concatenate([stay[chunk], held[step, chunk]], axis=0)

        for chunk in range(col_chunks):
            sent[step, chunk] = dot_nn(low, pair(chunk))
            ring_copy(step, chunk).start()

        @pl.when(step > 0)
        def _():
            for chunk in range(col_chunks, chunks):
                ring_copy(step - 1, chunk).wait_recv()

        for chunk in range(col_chunks, chunks):
            sent[step, chunk] = dot_nn(low, pair(chunk))
            ring_copy(step, chunk).start()
        for chunk in range(chunks):
            stay[chunk] = dot_nn(top, pair(chunk))
        stay_gram[...] = dot_nt(dot_nn(top, g), top)

        @pl.when(step < STEPS - 1)
        def _():
            total = jnp.zeros((half, order), jnp.float32)
            for chunk in range(col_chunks):
                ring_copy(step, chunk).wait_recv()
                moving = held[step + 1, chunk]
                total = total + dot_nt(moving, jnp.concatenate([stay[chunk], moving], axis=0))
            grams[step + 1, row_place, half:, :] = total
            for off in range(1, peers):
                gram_copy(step + 1, off, False).start()

        for chunk in range(chunks):
            ring_copy(step, chunk).wait_send()
        return carry

    lax.fori_loop(0, STEPS, advance, 0)
    for chunk in range(chunks):
        ring_copy(STEPS - 1, chunk).wait_recv()
        target = new_columns if chunk < col_chunks else new_factor
        at = lanes(chunk if chunk < col_chunks else chunk - col_chunks)
        target[:half, at] = stay[chunk]
        target[half:, at] = held[STEPS, chunk]


def body(columns, right_factor):
    order = columns.shape[0]
    half = order // 2
    chunks = (columns.shape[1] + right_factor.shape[1]) // LANES
    peers = lax.axis_size("rows")
    return pl.pallas_call(
        cycle_kernel,
        out_shape=[jax.ShapeDtypeStruct(a.shape, a.dtype) for a in (columns, right_factor)],
        in_specs=[pl.BlockSpec(memory_space=pltpu.VMEM)] * 2,
        out_specs=[pl.BlockSpec(memory_space=pltpu.VMEM)] * 2,
        scratch_shapes=[
            pltpu.VMEM((chunks, half, LANES), jnp.float32),
            pltpu.VMEM((STEPS, chunks, half, LANES), jnp.float32),
            pltpu.VMEM((STEPS + 1, chunks, half, LANES), jnp.float32),
            pltpu.VMEM((STEPS, peers, order, order), jnp.float32),
            pltpu.VMEM((half, half), jnp.float32),
            pltpu.VMEM((order, order), jnp.float32),
            pltpu.VMEM((order, order), jnp.float32),
            pltpu.VMEM((order, 2 * order), jnp.float32),
            pltpu.SemaphoreType.DMA((STEPS, chunks)),
            pltpu.SemaphoreType.DMA((STEPS, chunks)),
            pltpu.SemaphoreType.DMA((STEPS, peers - 1)),
            pltpu.SemaphoreType.DMA((STEPS, peers - 1)),
        ],
        compiler_params=pltpu.CompilerParams(collective_id=0, has_side_effects=True),
        name="cycle",
    )(columns, right_factor)


def solution(mesh):
    return jax.shard_map(
        body,
        mesh=mesh,
        in_specs=(P("blk", "rows"), P("blk", "rows")),
        out_specs=(P("blk", "rows"), P("blk", "rows")),
        check_vma=False,
    )
```

```python
import jax
import jax.numpy as jnp
from jax import lax
from jax.experimental import pallas as pl
from jax.experimental.pallas import tpu as pltpu
from jax.sharding import PartitionSpec as P

STEPS = 6
PANEL = 16
LANES = 128
MESH = pl.DeviceIdType.MESH

HIGHEST_PREC = lax.Precision.HIGHEST


def dot_nn(a, b):
    return lax.dot_general(
        a, b, (((1,), (0,)), ((), ())), precision=HIGHEST_PREC, preferred_element_type=jnp.float32
    )


def dot_nt(a, b):
    return lax.dot_general(
        a, b, (((1,), (1,)), ((), ())), precision=HIGHEST_PREC, preferred_element_type=jnp.float32
    )


def dot_tn(a, b):
    return lax.dot_general(
        a, b, (((0,), (0,)), ((), ())), precision=HIGHEST_PREC, preferred_element_type=jnp.float32
    )


def eliminate(work, midway=None):
    order, width = work.shape
    panels = order // PANEL
    for panel in range(panels):
        if midway is not None and panel == panels // 2 - 1:
            midway()
        low = panel * PANEL
        high = low + PANEL
        end = min(high + PANEL, order)
        rows = work[low:high, :]
        below = work[high:end, :] if end > high else None
        spread = [
            jnp.broadcast_to(rows[:, low + k : low + k + 1], (PANEL, 128)) for k in range(PANEL)
        ]
        spread_below = None
        if below is not None:
            spread_below = [
                jnp.broadcast_to(below[:, low + k : low + k + 1], (end - high, 128))
                for k in range(PANEL)
            ]
        done = []
        for j in range(PANEL):
            scale = lax.rsqrt(spread[j][j : j + 1, :])
            column = spread[j] * scale
            wide = jnp.concatenate([scale] * (width // 128), axis=1)
            pivot_row = rows[j : j + 1, :] * wide
            done.append(pivot_row)
            wide_column = jnp.concatenate([column] * (width // 128), axis=1)
            if j + 1 < PANEL:
                rows = rows - wide_column * pivot_row
            if below is not None:
                column_below = spread_below[j] * scale
                wide_below = jnp.concatenate([column_below] * (width // 128), axis=1)
                below = below - wide_below * pivot_row
            for k in range(j + 1, PANEL):
                head = spread[k][j : j + 1, :] * scale
                spread[k] = spread[k] - column * head
                if below is not None:
                    spread_below[k] = spread_below[k] - column_below * head
        finished = jnp.concatenate(done, axis=0)
        work[low:high, :] = finished
        if below is not None:
            work[high:end, :] = below
        if end < order:
            work[end:, :] = work[end:, :] - dot_tn(finished[:, end:order], finished)


def lanes(chunk):
    return slice(chunk * LANES, (chunk + 1) * LANES)


def cycle_kernel(
    columns, right_factor, new_columns, new_factor, own, near, stay_fac, sent_fac, held_fac, grams,
    near_grams, lows, near_lows, cross, work, solve, pair_sent, pair_sem, fac_sent, fac_sem, gram_sent,
    gram_sem, low_sent, low_sem, cross_sent, cross_sem,
):
    half = columns.shape[0] // 2
    order = 2 * half
    col_chunks = columns.shape[1] // LANES
    fac_chunks = right_factor.shape[1] // LANES
    ring, peers = lax.axis_size("blk"), lax.axis_size("rows")
    place, row_place = lax.axis_index("blk"), lax.axis_index("rows")
    right, left = lax.rem(place + 1, ring), lax.rem(place + ring - 1, ring)

    barrier = pltpu.get_barrier_semaphore()
    for neighbour in (left, right):
        pl.semaphore_signal(barrier, inc=1, device_id={"blk": neighbour}, device_id_type=MESH)
    for off in range(1, peers):
        peer = lax.rem(row_place + off, peers)
        pl.semaphore_signal(barrier, inc=1, device_id={"rows": peer}, device_id_type=MESH)

    def to_right(source, target, send_sem, recv_sem):
        return pltpu.make_async_remote_copy(
            src_ref=source,
            dst_ref=target,
            send_sem=send_sem,
            recv_sem=recv_sem,
            device_id={"blk": right},
            device_id_type=MESH,
        )

    def pair_copy(step, chunk):
        return to_right(
            own.at[step, chunk], near.at[step, chunk], pair_sent.at[step, chunk], pair_sem.at[step, chunk]
        )

    def fac_copy(step, chunk):
        return to_right(
            sent_fac.at[step, chunk],
            held_fac.at[step + 1, chunk],
            fac_sent.at[step, chunk],
            fac_sem.at[step, chunk],
        )

    def gram_copy(step):
        return to_right(grams.at[step], near_grams.at[step], gram_sent.at[step], gram_sem.at[step])

    def low_copy(step):
        return to_right(lows.at[step], near_lows.at[step], low_sent.at[step], low_sem.at[step])

    def cross_copy(slot, off):
        part = cross.at[slot, row_place]
        return pltpu.make_async_remote_copy(
            src_ref=part,
            dst_ref=part,
            send_sem=cross_sent.at[slot, off - 1],
            recv_sem=cross_sem.at[slot, off - 1],
            device_id={"rows": lax.rem(row_place + off, peers)},
            device_id_type=MESH,
        )

    def cross_sum(slot):
        total = cross[slot, 0]
        for peer in range(1, peers):
            total = total + cross[slot, peer]
        return total

    total = jnp.zeros((order, order), jnp.float32)
    for chunk in range(col_chunks):
        part = columns[:, lanes(chunk)]
        own[0, chunk] = part
        total = total + dot_nt(part, part)
    cross[0, row_place] = total
    for chunk in range(fac_chunks):
        stay_fac[chunk] = right_factor[:half, lanes(chunk)]
        held_fac[0, chunk] = right_factor[half:, lanes(chunk)]
    pl.semaphore_wait(barrier, 2 + peers - 1)
    for off in range(1, peers):
        cross_copy(0, off).start()
    for chunk in range(col_chunks):
        pair_copy(0, chunk).start()
    for off in range(1, peers):
        cross_copy(0, off).wait()
    grams[0] = cross_sum(0)

    def advance(step, carry):
        gram_copy(step).start()
        g = grams[step]
        work[...] = dot_nn(g, g)
        eliminate(work)
        upper = work[...]
        keep = lax.broadcasted_iota(jnp.int32, upper.shape, 0) <= lax.broadcasted_iota(
            jnp.int32, upper.shape, 1
        )
        upper = jnp.where(keep, upper, 0.0)
        solve[:, :order] = dot_nt(upper, upper)
        solve[:, order:] = upper

        def products():
            for chunk in range(col_chunks):
                pair_copy(step, chunk).wait_recv()

            @pl.when(step < STEPS - 1)
            def _():
                total = jnp.zeros((order, order), jnp.float32)
                for chunk in range(col_chunks):
                    total = total + dot_nt(own[step, chunk], near[step, chunk])
                cross[step + 1, row_place] = total
                for off in range(1, peers):
                    cross_copy(step + 1, off).start()

        eliminate(solve, products)
        turn = solve[:, order:]
        top, low = turn[:half], turn[half:]
        lows[step] = low
        low_copy(step).start()

        for chunk in range(col_chunks):
            own[step + 1, chunk, :half] = dot_nn(top, own[step, chunk])

        @pl.when(step > 0)
        def _():
            for chunk in range(fac_chunks):
                fac_copy(step - 1, chunk).wait_recv()

        for chunk in range(fac_chunks):
            turned = dot_nn(turn, jnp.concatenate([stay_fac[chunk], held_fac[step, chunk]], axis=0))
            stay_fac[chunk] = turned[:half]
            sent_fac[step, chunk] = turned[half:]
            fac_copy(step, chunk).start()
        gram_copy(step).wait_recv()

        @pl.when(step < STEPS - 1)
        def _():
            grams[step + 1, :half, :half] = dot_nt(dot_nn(top, grams[step]), top)
            for off in range(1, peers):
                cross_copy(step + 1, off).wait()
            reach = dot_nn(top, cross_sum(step + 1))
            low_copy(step).wait_recv()
            arrived = near_lows[step]
            term = dot_nt(reach, arrived)
            grams[step + 1, :half, half:] = term
            grams[step + 1, half:, :half] = term.T
            grams[step + 1, half:, half:] = dot_nt(dot_nn(arrived, near_grams[step]), arrived)
            for chunk in range(col_chunks):
                own[step + 1, chunk, half:] = dot_nn(arrived, near[step, chunk])
                pair_copy(step + 1, chunk).start()

        for chunk in range(col_chunks):
            pair_copy(step, chunk).wait_send()
        for chunk in range(fac_chunks):
            fac_copy(step, chunk).wait_send()
        gram_copy(step).wait_send()
        low_copy(step).wait_send()
        return carry

    lax.fori_loop(0, STEPS, advance, 0)
    low_copy(STEPS - 1).wait_recv()
    for chunk in range(col_chunks):
        new_columns[:half, lanes(chunk)] = own[STEPS, chunk, :half]
        new_columns[half:, lanes(chunk)] = dot_nn(near_lows[STEPS - 1], near[STEPS - 1, chunk])
    for chunk in range(fac_chunks):
        fac_copy(STEPS - 1, chunk).wait_recv()
        new_factor[:half, lanes(chunk)] = stay_fac[chunk]
        new_factor[half:, lanes(chunk)] = held_fac[STEPS, chunk]


def body(columns, right_factor):
    order = columns.shape[0]
    half = order // 2
    col_chunks = columns.shape[1] // LANES
    fac_chunks = right_factor.shape[1] // LANES
    peers = lax.axis_size("rows")

    def room(*shape):
        return pltpu.VMEM(shape, jnp.float32)

    return pl.pallas_call(
        cycle_kernel,
        out_shape=[jax.ShapeDtypeStruct(a.shape, a.dtype) for a in (columns, right_factor)],
        in_specs=[pl.BlockSpec(memory_space=pltpu.VMEM)] * 2,
        out_specs=[pl.BlockSpec(memory_space=pltpu.VMEM)] * 2,
        scratch_shapes=[
            room(STEPS + 1, col_chunks, order, LANES),
            room(STEPS, col_chunks, order, LANES),
            room(fac_chunks, half, LANES),
            room(STEPS, fac_chunks, half, LANES),
            room(STEPS + 1, fac_chunks, half, LANES),
            room(STEPS, order, order),
            room(STEPS, order, order),
            room(STEPS, half, order),
            room(STEPS, half, order),
            room(STEPS, peers, order, order),
            room(order, order),
            room(order, 2 * order),
            pltpu.SemaphoreType.DMA((STEPS, col_chunks)),
            pltpu.SemaphoreType.DMA((STEPS, col_chunks)),
            pltpu.SemaphoreType.DMA((STEPS, fac_chunks)),
            pltpu.SemaphoreType.DMA((STEPS, fac_chunks)),
            pltpu.SemaphoreType.DMA((STEPS,)),
            pltpu.SemaphoreType.DMA((STEPS,)),
            pltpu.SemaphoreType.DMA((STEPS,)),
            pltpu.SemaphoreType.DMA((STEPS,)),
            pltpu.SemaphoreType.DMA((STEPS, peers - 1)),
            pltpu.SemaphoreType.DMA((STEPS, peers - 1)),
        ],
        compiler_params=pltpu.CompilerParams(collective_id=0, has_side_effects=True),
        name="cycle",
    )(columns, right_factor)


def solution(mesh):
    return jax.shard_map(
        body,
        mesh=mesh,
        in_specs=(P("blk", "rows"), P("blk", "rows")),
        out_specs=(P("blk", "rows"), P("blk", "rows")),
        check_vma=False,
    )
```

```python
import jax
import jax.numpy as jnp
from jax import lax
from jax.experimental import pallas as pl
from jax.experimental.pallas import tpu as pltpu
from jax.sharding import PartitionSpec as P

STEPS = 6
PANEL = 16
LANES = 128
MESH = pl.DeviceIdType.MESH

HIGHEST_PREC = lax.Precision.HIGHEST


def dot_nn(a, b):
    return lax.dot_general(
        a, b, (((1,), (0,)), ((), ())), precision=HIGHEST_PREC, preferred_element_type=jnp.float32
    )


def dot_nt(a, b):
    return lax.dot_general(
        a, b, (((1,), (1,)), ((), ())), precision=HIGHEST_PREC, preferred_element_type=jnp.float32
    )


def dot_tn(a, b):
    return lax.dot_general(
        a, b, (((0,), (0,)), ((), ())), precision=HIGHEST_PREC, preferred_element_type=jnp.float32
    )


def eliminate(work, midway=None):
    order, width = work.shape
    panels = order // PANEL
    for panel in range(panels):
        if midway is not None and panel == panels // 2 - 1:
            midway()
        low = panel * PANEL
        high = low + PANEL
        end = min(high + PANEL, order)
        rows = work[low:high, :]
        below = work[high:end, :] if end > high else None
        spread = [
            jnp.broadcast_to(rows[:, low + k : low + k + 1], (PANEL, 128)) for k in range(PANEL)
        ]
        spread_below = None
        if below is not None:
            spread_below = [
                jnp.broadcast_to(below[:, low + k : low + k + 1], (end - high, 128))
                for k in range(PANEL)
            ]
        done = []
        for j in range(PANEL):
            scale = lax.rsqrt(spread[j][j : j + 1, :])
            column = spread[j] * scale
            wide = jnp.concatenate([scale] * (width // 128), axis=1)
            pivot_row = rows[j : j + 1, :] * wide
            done.append(pivot_row)
            wide_column = jnp.concatenate([column] * (width // 128), axis=1)
            if j + 1 < PANEL:
                rows = rows - wide_column * pivot_row
            if below is not None:
                column_below = spread_below[j] * scale
                wide_below = jnp.concatenate([column_below] * (width // 128), axis=1)
                below = below - wide_below * pivot_row
            for k in range(j + 1, PANEL):
                head = spread[k][j : j + 1, :] * scale
                spread[k] = spread[k] - column * head
                if below is not None:
                    spread_below[k] = spread_below[k] - column_below * head
        finished = jnp.concatenate(done, axis=0)
        work[low:high, :] = finished
        if below is not None:
            work[high:end, :] = below
        if end < order:
            work[end:, :] = work[end:, :] - dot_tn(finished[:, end:order], finished)


def lanes(chunk):
    return slice(chunk * LANES, (chunk + 1) * LANES)


def cycle_kernel(
    columns, right_factor, new_columns, new_factor, own, near, stay_fac, sent_fac, held_fac, grams,
    near_grams, lows, near_lows, cross, work, solve, pair_sent, pair_sem, fac_sent, fac_sem, gram_sent,
    gram_sem, low_sent, low_sem, cross_sent, cross_sem,
):
    half = columns.shape[0] // 2
    order = 2 * half
    col_chunks = columns.shape[1] // LANES
    fac_chunks = right_factor.shape[1] // LANES
    ring, peers = lax.axis_size("blk"), lax.axis_size("rows")
    place, row_place = lax.axis_index("blk"), lax.axis_index("rows")
    right, left = lax.rem(place + 1, ring), lax.rem(place + ring - 1, ring)

    barrier = pltpu.get_barrier_semaphore()
    for neighbour in (left, right):
        pl.semaphore_signal(barrier, inc=1, device_id={"blk": neighbour}, device_id_type=MESH)
    for off in range(1, peers):
        peer = lax.rem(row_place + off, peers)
        pl.semaphore_signal(barrier, inc=1, device_id={"rows": peer}, device_id_type=MESH)

    def to_right(source, target, send_sem, recv_sem):
        return pltpu.make_async_remote_copy(
            src_ref=source,
            dst_ref=target,
            send_sem=send_sem,
            recv_sem=recv_sem,
            device_id={"blk": right},
            device_id_type=MESH,
        )

    def pair_copy(step, chunk):
        return to_right(
            own.at[step, chunk], near.at[step, chunk], pair_sent.at[step, chunk], pair_sem.at[step, chunk]
        )

    def fac_copy(step, chunk):
        return to_right(
            sent_fac.at[step, chunk],
            held_fac.at[step + 1, chunk],
            fac_sent.at[step, chunk],
            fac_sem.at[step, chunk],
        )

    def gram_copy(step):
        return to_right(grams.at[step], near_grams.at[step], gram_sent.at[step], gram_sem.at[step])

    def low_copy(step):
        return to_right(lows.at[step], near_lows.at[step], low_sent.at[step], low_sem.at[step])

    def cross_copy(slot, off):
        part = cross.at[slot, row_place]
        return pltpu.make_async_remote_copy(
            src_ref=part,
            dst_ref=part,
            send_sem=cross_sent.at[slot, off - 1],
            recv_sem=cross_sem.at[slot, off - 1],
            device_id={"rows": lax.rem(row_place + off, peers)},
            device_id_type=MESH,
        )

    def cross_sum(slot):
        total = cross[slot, 0]
        for peer in range(1, peers):
            total = total + cross[slot, peer]
        return total

    total = jnp.zeros((order, order), jnp.float32)
    for chunk in range(col_chunks):
        part = columns[:, lanes(chunk)]
        own[0, chunk] = part
        total = total + dot_nt(part, part)
    cross[0, row_place] = total
    for chunk in range(fac_chunks):
        stay_fac[chunk] = right_factor[:half, lanes(chunk)]
        held_fac[0, chunk] = right_factor[half:, lanes(chunk)]
    pl.semaphore_wait(barrier, 2 + peers - 1)
    for off in range(1, peers):
        cross_copy(0, off).start()
    for chunk in range(col_chunks):
        pair_copy(0, chunk).start()
    for off in range(1, peers):
        cross_copy(0, off).wait()
    grams[0] = cross_sum(0)

    def advance(step, carry):
        gram_copy(step).start()
        g = grams[step]
        work[...] = dot_nn(g, g)
        eliminate(work)
        upper = work[...]
        keep = lax.broadcasted_iota(jnp.int32, upper.shape, 0) <= lax.broadcasted_iota(
            jnp.int32, upper.shape, 1
        )
        upper = jnp.where(keep, upper, 0.0)
        solve[:, :order] = dot_nt(upper, upper)
        solve[:, order:] = upper

        def products():
            for chunk in range(col_chunks):
                pair_copy(step, chunk).wait_recv()

            @pl.when(step < STEPS - 1)
            def _():
                total = jnp.zeros((order, order), jnp.float32)
                for chunk in range(col_chunks):
                    total = total + dot_nt(own[step, chunk], near[step, chunk])
                cross[step + 1, row_place] = total
                for off in range(1, peers):
                    cross_copy(step + 1, off).start()

        eliminate(solve, products)
        turn = solve[:, order:]
        top, low = turn[:half], turn[half:]
        lows[step] = low
        low_copy(step).start()

        for chunk in range(col_chunks):
            own[step + 1, chunk, :half] = dot_nn(top, own[step, chunk])

        @pl.when(step > 0)
        def _():
            for chunk in range(fac_chunks):
                fac_copy(step - 1, chunk).wait_recv()

        for chunk in range(fac_chunks):
            turned = dot_nn(turn, jnp.concatenate([stay_fac[chunk], held_fac[step, chunk]], axis=0))
            stay_fac[chunk] = turned[:half]
            sent_fac[step, chunk] = turned[half:]
            fac_copy(step, chunk).start()
        gram_copy(step).wait_recv()

        @pl.when(step < STEPS - 1)
        def _():
            grams[step + 1, :half, :half] = dot_nt(dot_nn(top, grams[step]), top)
            for off in range(1, peers):
                cross_copy(step + 1, off).wait()
            reach = dot_nn(top, cross_sum(step + 1))
            low_copy(step).wait_recv()
            arrived = near_lows[step]
            grams[step + 1, :half, half:] = dot_nt(reach, arrived)
            grams[step + 1, half:, :half] = dot_nt(arrived, reach)
            grams[step + 1, half:, half:] = dot_nt(dot_nn(arrived, near_grams[step]), arrived)
            for chunk in range(col_chunks):
                own[step + 1, chunk, half:] = dot_nn(arrived, near[step, chunk])
                pair_copy(step + 1, chunk).start()

        return carry

    lax.fori_loop(0, STEPS, advance, 0)
    low_copy(STEPS - 1).wait_recv()
    for chunk in range(col_chunks):
        new_columns[:half, lanes(chunk)] = own[STEPS, chunk, :half]
        new_columns[half:, lanes(chunk)] = dot_nn(near_lows[STEPS - 1], near[STEPS - 1, chunk])
    for chunk in range(fac_chunks):
        fac_copy(STEPS - 1, chunk).wait_recv()
        new_factor[:half, lanes(chunk)] = stay_fac[chunk]
        new_factor[half:, lanes(chunk)] = held_fac[STEPS, chunk]

    def settle(step, carry):
        for chunk in range(col_chunks):
            pair_copy(step, chunk).wait_send()
        for chunk in range(fac_chunks):
            fac_copy(step, chunk).wait_send()
        gram_copy(step).wait_send()
        low_copy(step).wait_send()
        return carry

    lax.fori_loop(0, STEPS, settle, 0)


def body(columns, right_factor):
    order = columns.shape[0]
    half = order // 2
    col_chunks = columns.shape[1] // LANES
    fac_chunks = right_factor.shape[1] // LANES
    peers = lax.axis_size("rows")

    def room(*shape):
        return pltpu.VMEM(shape, jnp.float32)

    return pl.pallas_call(
        cycle_kernel,
        out_shape=[jax.ShapeDtypeStruct(a.shape, a.dtype) for a in (columns, right_factor)],
        in_specs=[pl.BlockSpec(memory_space=pltpu.VMEM)] * 2,
        out_specs=[pl.BlockSpec(memory_space=pltpu.VMEM)] * 2,
        scratch_shapes=[
            room(STEPS + 1, col_chunks, order, LANES),
            room(STEPS, col_chunks, order, LANES),
            room(fac_chunks, half, LANES),
            room(STEPS, fac_chunks, half, LANES),
            room(STEPS + 1, fac_chunks, half, LANES),
            room(STEPS, order, order),
            room(STEPS, order, order),
            room(STEPS, half, order),
            room(STEPS, half, order),
            room(STEPS, peers, order, order),
            room(order, order),
            room(order, 2 * order),
            pltpu.SemaphoreType.DMA((STEPS, col_chunks)),
            pltpu.SemaphoreType.DMA((STEPS, col_chunks)),
            pltpu.SemaphoreType.DMA((STEPS, fac_chunks)),
            pltpu.SemaphoreType.DMA((STEPS, fac_chunks)),
            pltpu.SemaphoreType.DMA((STEPS,)),
            pltpu.SemaphoreType.DMA((STEPS,)),
            pltpu.SemaphoreType.DMA((STEPS,)),
            pltpu.SemaphoreType.DMA((STEPS,)),
            pltpu.SemaphoreType.DMA((STEPS, peers - 1)),
            pltpu.SemaphoreType.DMA((STEPS, peers - 1)),
        ],
        compiler_params=pltpu.CompilerParams(collective_id=0, has_side_effects=True),
        name="cycle",
    )(columns, right_factor)


def solution(mesh):
    return jax.shard_map(
        body,
        mesh=mesh,
        in_specs=(P("blk", "rows"), P("blk", "rows")),
        out_specs=(P("blk", "rows"), P("blk", "rows")),
        check_vma=False,
    )
```
